16 devices in a mesh: dp: 1, tp: 16 (over x, y, z, core).
Axes of the slice: x: 2, y: 2, z: 2, core: 2. Of those that a mesh axis runs over, the one named last changes fastest.
Arguments:
- x: bfloat16 [2048, 14336], P(('dp', 'tp'))
- dy: bfloat16 [2048, 14336], P(('dp', 'tp'))
- gain: bfloat16 [14336], replicated
- wq: bfloat16 [14336, 14336], P(None, 'tp')
- wk: bfloat16 [14336, 14336], P(None, 'tp')
- wv: bfloat16 [14336, 14336], P(None, 'tp')
- wo: bfloat16 [14336, 14336], P('tp')
Outputs:
- output 1: bfloat16 [2048, 14336], P(('dp', 'tp'))
- output 2: float32 [1, 14336], P('dp')
- output 3: bfloat16 [14336, 14336], P('dp', 'tp')
- output 4: bfloat16 [14336, 14336], P('dp', 'tp')
- output 5: bfloat16 [14336, 14336], P('dp', 'tp')
- output 6: bfloat16 [14336, 14336], P(('dp', 'tp'))
All inputs are finite; a program needn't handle non-finite values.
Results may differ from the reference program's by a relative error of at most 0.018.
Values are sent between devices in bfloat16 or wider.
A program may use at most 2 GiB of HBM per device.

```python
import jax
import jax.numpy as jnp
from jax import lax

ROWS = 2048
D = 14336
HEADS = 112
KV_HEADS = 112
HEAD = 128
THETA = 10000


def setup_inputs(seed: int = 0, part: int = 0) -> dict:
    kx, ky, kn, kq, kk, kv, ko = jax.random.split(jax.random.key(seed), 7)

    def weights(key, rows, columns):
        return jax.random.normal(key, (rows, columns), jnp.float32) * rows**-0.5

    drawn = {
        "x": jax.random.normal(jax.random.fold_in(kx, part), (ROWS, D), jnp.float32),
        "dy": jax.random.normal(jax.random.fold_in(ky, part), (ROWS, D), jnp.float32) * ROWS**-0.5,
        "gain": 1 + 0.1 * jax.random.normal(kn, (D,), jnp.float32),
        "wq": 2 * weights(kq, D, HEADS * HEAD),
        "wk": 2 * weights(kk, D, KV_HEADS * HEAD),
        "wv": 4 * weights(kv, D, KV_HEADS * HEAD),
        "wo": weights(ko, HEADS * HEAD, D),
    }
    return {k: v.astype(jnp.bfloat16) for k, v in drawn.items()}


def normed(x, gain):
    wide = x.astype(jnp.float32)
    scale = lax.rsqrt(jnp.mean(wide * wide, -1, keepdims=True) + 1e-6)
    return (wide * scale * gain.astype(jnp.float32)).astype(jnp.bfloat16)


def turned(t, place, theta):
    half = t.shape[-1] // 2
    angle = place.astype(jnp.float32)[:, None] * theta ** (-jnp.arange(half, dtype=jnp.float32) / half)
    cos, sin = jnp.cos(angle)[:, None], jnp.sin(angle)[:, None]
    a, b = t[..., :half].astype(jnp.float32), t[..., half:].astype(jnp.float32)
    return jnp.concatenate([a * cos - b * sin, b * cos + a * sin], -1).astype(jnp.bfloat16)


def matmul(a, w):
    return jnp.dot(a, w, preferred_element_type=jnp.float32).astype(jnp.bfloat16)


def einsum(form, a, b):
    return jnp.einsum(form, a.astype(jnp.float32), b.astype(jnp.float32))


def attention(q, k, v):
    scores = einsum("tgsd,ugd->gstu", q, k) * q.shape[-1] ** -0.5
    token = jnp.arange(q.shape[0])
    scores = jnp.where(token[:, None] >= token, scores, -jnp.inf)
    weights = jax.nn.softmax(scores, -1).astype(jnp.bfloat16)
    return einsum("gstu,ugd->tgsd", weights, v).astype(jnp.bfloat16)


def forward(x, gain, wq, wk, wv, wo):
    rows = x.shape[0]
    a, place = normed(x, gain), jnp.arange(rows)
    k = turned(matmul(a, wk).reshape(rows, -1, HEAD), place, THETA)
    q = turned(matmul(a, wq).reshape(rows, -1, HEAD), place, THETA).reshape(rows, k.shape[1], -1, HEAD)
    v = matmul(a, wv).reshape(rows, -1, HEAD)
    seen = attention(q, k, v).reshape(rows, -1)
    return (x.astype(jnp.float32) + jnp.dot(seen, wo, preferred_element_type=jnp.float32)).astype(jnp.bfloat16)


def reference(x, dy, gain, wq, wk, wv, wo):
    _, back = jax.vjp(forward, x, gain.astype(jnp.float32), wq, wk, wv, wo)
    by_x, by_gain, *by_weights = back(dy)
    return (by_x, by_gain[None], *by_weights)
```

```python
import functools

import jax
import jax.numpy as jnp
from jax import lax
from jax.experimental import pallas as pl
from jax.experimental.pallas import tpu as pltpu
from jax.sharding import PartitionSpec as P


HEAD = 128
THETA = 10000
NEG = -1e30
HIDDEN = 2 * NEG
LOG2E = 1.4426950408889634
VMEM = 60 * 2**20
BLOCK = 512
ROUTES = ((2, 4, 8), (4, 8, 2), (8, 2, 4))


def _dot(a, b, ca, cb):
    return lax.dot_general(a, b, (((ca,), (cb,)), ((), ())), preferred_element_type=jnp.float32)


def _params(n=1):
    return pltpu.CompilerParams(dimension_semantics=("arbitrary",) * n, vmem_limit_bytes=VMEM)


def _cost(flops, arrays, trans=0):
    return pl.CostEstimate(flops=int(flops), transcendentals=int(trans), bytes_accessed=int(sum(a.size * a.dtype.itemsize for a in arrays)))


def _swap(t, cos, sin):
    return t * cos + pltpu.roll(t, HEAD // 2, 1) * sin


def _project(pos_ref, *refs, sizes, n_w, turn, contract):
    n = len(sizes)
    pieces, weights = refs[:n], refs[n : n + n_w]
    rest = refs[n + n_w :]
    cos_ref, sin_ref = (rest[0], rest[1]) if turn else (None, None)
    out_ref, whole_ref, acc, held, sems, out_sems = rest[-6:]
    k, last = pl.program_id(0), pl.num_programs(0) - 1
    bk = pieces[0].shape[1]
    starts = [sum(sizes[:i]) for i in range(n)]
    copies = [
        pltpu.make_async_copy(p, whole_ref.at[pl.ds(pl.multiple_of(pos_ref[i], 16), s), pl.ds(pl.multiple_of(k * bk, bk), bk)], sems.at[i])
        for i, (p, s) in enumerate(zip(pieces, sizes))
    ]
    for c in copies:
        c.start()
    rows = jnp.concatenate([p[...] for p in pieces], axis=0)
    w = jnp.concatenate([w[...] for w in weights], axis=1) if n_w > 1 else weights[0][...]

    def term():
        return _dot(w, rows, 1, 1) if contract else _dot(rows, w, 1, 0)

    @pl.when(k == 0)
    def _():
        acc[...] = term()

    @pl.when(k > 0)
    def _():
        acc[...] += term()

    @pl.when(k == last)
    def _():
        for h in range(held.shape[1] // HEAD):
            cols = slice(h * HEAD, (h + 1) * HEAD)
            t = (acc[cols, :].T if contract else acc[:, cols]).astype(jnp.bfloat16)
            if turn and h < turn:
                t = _swap(t.astype(jnp.float32), cos_ref[...], sin_ref[...]).astype(jnp.bfloat16)
            held[:, cols] = t
        outs = [
            pltpu.make_async_copy(held.at[pl.ds(at, s), :], out_ref.at[pl.ds(pl.multiple_of(pos_ref[i], 16), s), :], out_sems.at[i])
            for i, (at, s) in enumerate(zip(starts, sizes))
        ]
        for c in outs:
            c.start()
        for c in outs:
            c.wait()

    for c in copies:
        c.wait()


def project(pieces, pos, weights, out, whole, angles=None, transposed=False, bk=1024):
    sizes = tuple(p.shape[0] for p in pieces)
    rows, d = sum(sizes), pieces[0].shape[1]
    n_w, width = len(weights), weights[0].shape[0 if transposed else 1]
    cols = n_w * width
    turn = 2 * width // HEAD if angles is not None else 0
    in_specs = [pl.BlockSpec((s, bk), lambda k, _: (0, k)) for s in sizes]
    in_specs += [pl.BlockSpec((width, bk), lambda k, _: (0, k)) if transposed else pl.BlockSpec((bk, width), lambda k, _: (k, 0))] * n_w
    given = [*pieces, *weights]
    if angles is not None:
        in_specs += [pl.BlockSpec((rows, HEAD), lambda k, _: (0, 0))] * 2
        given += list(angles)
    shapes = [jax.ShapeDtypeStruct((16 * 128, cols), jnp.bfloat16), jax.ShapeDtypeStruct((16 * 128, d), jnp.bfloat16)]
    alias = {}
    if out is not None:
        alias = {1 + len(given): 0, 2 + len(given): 1}
        given += [out, whole]
        in_specs += [pl.BlockSpec(memory_space=pl.ANY)] * 2
    return pl.pallas_call(
        functools.partial(_project, sizes=sizes, n_w=n_w, turn=turn, contract=1 if transposed else 0),
        grid_spec=pltpu.PrefetchScalarGridSpec(
            num_scalar_prefetch=1,
            grid=(d // bk),
            in_specs=in_specs,
            out_specs=[pl.BlockSpec(memory_space=pl.ANY)] * 2,
            scratch_shapes=[pltpu.VMEM((cols, rows) if transposed else (rows, cols), jnp.float32), pltpu.VMEM((rows, cols), jnp.bfloat16),
                            pltpu.SemaphoreType.DMA((len(sizes),)), pltpu.SemaphoreType.DMA((len(sizes),))],
        ),
        out_shape=shapes,
        input_output_aliases=alias,
        compiler_params=_params(),
        cost_estimate=_cost(2 * rows * d * cols, [*pieces, *weights]),
        name="project_turn" if turn else "project",
    )(pos, *given)


def _attend(q_ref, k_ref, v_ref, o_ref, lse_ref, top_s, mix_s, *, heads, scale):
    iq = pl.program_id(0)
    e = scale * LOG2E
    low = k_ref.dtype
    ones = jnp.ones((8, BLOCK), low)
    top_s[...] = jnp.full_like(top_s, NEG)
    mix_s[...] = jnp.zeros_like(mix_s)
    cols = [slice(i * HEAD, (i + 1) * HEAD) for i in range(heads)]

    def block(j, masked):
        here = pl.ds(pl.multiple_of(j * BLOCK, BLOCK), BLOCK)
        scores = [_dot(k_ref[here, c], q_ref[:, c], 1, 1) for c in cols]
        if masked:
            ok = lax.broadcasted_iota(jnp.int32, (BLOCK, BLOCK), 1) >= lax.broadcasted_iota(jnp.int32, (BLOCK, BLOCK), 0)
        weights, keeps = [], []
        for i, s in enumerate(scores):
            if masked:
                s = jnp.where(ok, s, HIDDEN)
            old = top_s[i : i + 1, :]
            top = jnp.maximum(old, s.max(axis=0, keepdims=True))
            top_s[i : i + 1, :] = top
            weights.append(jnp.exp2((s - top) * e).astype(low))
            keeps.append(jnp.exp2((old - top) * e))
        for i, (p, keep) in enumerate(zip(weights, keeps)):
            values = jnp.concatenate([v_ref[here, cols[i]].T, ones], axis=0)
            mix_s[i] = mix_s[i] * keep + _dot(values, p, 1, 0)

    lax.fori_loop(0, iq, lambda j, _: block(j, False), None)
    block(iq, True)
    for i in range(heads):
        total = mix_s[i, HEAD : HEAD + 1, :]
        o_ref[:, cols[i]] = (mix_s[i, :HEAD, :] * (1 / total)).T.astype(o_ref.dtype)
        lse_ref[i] = top_s[i : i + 1, :] * scale + jnp.log(total)


def attend(qkv):
    rows, heads = qkv.shape[0], qkv.shape[1] // (3 * HEAD)
    wide = heads * HEAD
    pairs = heads * rows * (rows + BLOCK) // 2
    return pl.pallas_call(
        functools.partial(_attend, heads=heads, scale=HEAD**-0.5),
        grid=(rows // BLOCK),
        in_specs=[pl.BlockSpec((BLOCK, wide), lambda i: (i, 0)), pl.BlockSpec((rows, wide), lambda i: (0, 1)),
                  pl.BlockSpec((rows, wide), lambda i: (0, 2))],
        out_specs=[pl.BlockSpec((BLOCK, wide), lambda i: (i, 0)), pl.BlockSpec((heads, 1, BLOCK), lambda i: (0, 0, i))],
        out_shape=[jax.ShapeDtypeStruct((rows, wide), jnp.bfloat16), jax.ShapeDtypeStruct((heads, 1, rows), jnp.float32)],
        scratch_shapes=[pltpu.VMEM((8 * ((heads + 7) // 8), BLOCK), jnp.float32), pltpu.VMEM((heads, HEAD + 8, BLOCK), jnp.float32)],
        compiler_params=_params(),
        cost_estimate=_cost(4 * pairs * HEAD, [qkv], pairs),
        name="attend",
    )(qkv, qkv, qkv)


def _attend_back(q_ref, k_ref, v_ref, do_ref, o_ref, lse_ref, cos_ref, sin_ref, dq_ref, dk_ref, dv_ref, dq_s, dk_s, dv_s, *, scale):
    low = q_ref.dtype
    e = scale * LOG2E
    n = q_ref.shape[0] // BLOCK
    at = [slice(i * BLOCK, (i + 1) * BLOCK) for i in range(n)]
    lses = [lse_ref[0, :, a] * LOG2E for a in at]
    deltas = [(do_ref[a, :].astype(jnp.float32) * o_ref[a, :].astype(jnp.float32)).T.sum(axis=0, keepdims=True) for a in at]
    for j in range(n):
        k, v = k_ref[at[j], :], v_ref[at[j], :]
        kt = k.T
        scores = {i: _dot(k, q_ref[at[i], :], 1, 1) for i in range(j, n)}
        dps = {i: _dot(v, do_ref[at[i], :], 1, 1) for i in range(j, n)}
        for i in range(j, n):
            p = jnp.exp2(scores[i] * e - lses[i])
            if i == j:
                ok = lax.broadcasted_iota(jnp.int32, (BLOCK, BLOCK), 1) >= lax.broadcasted_iota(jnp.int32, (BLOCK, BLOCK), 0)
                p = jnp.where(ok, p, 0.0)
            ds = (p * (dps[i] - deltas[i])).astype(low)
            dv = _dot(p.astype(low), do_ref[at[i], :], 1, 0)
            dk = _dot(ds, q_ref[at[i], :], 1, 0)
            dq = _dot(kt, ds, 1, 0)
            if i == j:
                dv_s[...] = dv
                dk_s[...] = dk
            else:
                dv_s[...] += dv
                dk_s[...] += dk
            if j == 0:
                dq_s[:, at[i]] = dq
            else:
                dq_s[:, at[i]] += dq
        dv_ref[at[j], :] = dv_s[...].astype(low)
        back = (dk_s[...] * scale).astype(low).astype(jnp.float32)
        dk_ref[at[j], :] = _swap(back, cos_ref[at[j], :], -sin_ref[at[j], :]).astype(low)
        back = (dq_s[:, at[j]] * scale).T.astype(low).astype(jnp.float32)
        dq_ref[at[j], :] = _swap(back, cos_ref[at[j], :], -sin_ref[at[j], :]).astype(low)


def attend_back(qkv, d_out, out, lse, cos, sin):
    rows, wide = out.shape
    heads = wide // HEAD
    pairs = heads * rows * (rows + BLOCK) // 2
    column = lambda first: pl.BlockSpec((rows, HEAD), lambda h: (0, first + h))
    whole = pl.BlockSpec((rows, HEAD), lambda h: (0, 0))
    return pl.pallas_call(
        functools.partial(_attend_back, scale=HEAD**-0.5),
        grid=(heads),
        in_specs=[column(0), column(heads), column(2 * heads), column(0), column(0), pl.BlockSpec((1, 1, rows), lambda h: (h, 0, 0)), whole, whole],
        out_specs=[column(0)] * 3,
        out_shape=[jax.ShapeDtypeStruct((rows, wide), jnp.bfloat16)] * 3,
        scratch_shapes=[pltpu.VMEM((HEAD, rows), jnp.float32), pltpu.VMEM((BLOCK, HEAD), jnp.float32), pltpu.VMEM((BLOCK, HEAD), jnp.float32)],
        compiler_params=_params(),
        cost_estimate=_cost(10 * pairs * HEAD, [qkv, d_out, out], pairs),
        name="attend_back",
    )(qkv, qkv, qkv, d_out, out, lse, cos, sin)


def _by_rows(pos_ref, dq_ref, dk_ref, dv_ref, wq_ref, wk_ref, wv_ref, *rest, add):
    outs = rest[1:] if add else rest
    w = jnp.concatenate([w[...] for w in (wq_ref, wk_ref, wv_ref)], axis=1)
    per = outs[0].shape[0] // 128
    for o, out in enumerate(outs):
        take = [pl.ds(pl.multiple_of(pos_ref[o * per + i], 128), 128) for i in range(per)]
        rows = jnp.concatenate([jnp.concatenate([r[t, :] for r in (dq_ref, dk_ref, dv_ref)], axis=1) for t in take], axis=0)
        term = _dot(rows, w, 1, 1)
        if add:
            term = term + rest[0][o * per * 128 : (o + 1) * per * 128, :].astype(jnp.float32)
        out[...] = term.astype(out.dtype)


def by_rows(pos, grads, weights, first, width, bn, recv=None):
    rows, wide = grads[0].shape
    count = pos.shape[0]
    n_out = 2
    start = first // bn
    given = [*grads, *weights]
    in_specs = [pl.BlockSpec((rows, wide), lambda n, _: (0, 0))] * 3 + [pl.BlockSpec((bn, wide), lambda n, _: (start + n, 0))] * 3
    if recv is not None:
        given += [recv]
        in_specs += [pl.BlockSpec((count * 128, bn), lambda n, _: (0, n))]
    elif True:
        n_out = 1
    got = pl.pallas_call(
        functools.partial(_by_rows, add=recv is not None),
        grid_spec=pltpu.PrefetchScalarGridSpec(
            num_scalar_prefetch=1,
            grid=(width // bn),
            in_specs=in_specs,
            out_specs=[pl.BlockSpec((count * 128 // n_out, bn), lambda n, _: (0, n))] * n_out,
        ),
        out_shape=[jax.ShapeDtypeStruct((count * 128 // n_out, width), jnp.bfloat16)] * n_out,
        compiler_params=_params(),
        cost_estimate=_cost(2 * count * 128 * 3 * wide * width, given),
        name="by_rows",
    )(pos, *given)
    return got


def _by_weights(a_ref, dq_ref, dk_ref, dv_ref, *rest):
    grads = jnp.concatenate([r[...] for r in (dq_ref, dk_ref, dv_ref)], axis=1)
    got = _dot(a_ref[...], grads, 0, 0)
    outs = rest[-3:]
    wide = outs[0].shape[1]
    for i, o in enumerate(outs):
        o[...] = got[:, i * wide : (i + 1) * wide].astype(o.dtype)


def by_weights(a, grads, first, count, so_far, bm=512):
    rows, d = a.shape
    wide = grads[0].shape[1]
    given = [a, *grads]
    specs = [pl.BlockSpec((rows, bm), lambda m: (0, first + m))] + [pl.BlockSpec((rows, wide), lambda m: (0, 0))] * 3
    alias = {}
    if so_far is not None:
        given += so_far
        specs += [pl.BlockSpec(memory_space=pl.ANY)] * 3
        alias = {4: 0, 5: 1, 6: 2}
    return pl.pallas_call(
        _by_weights,
        grid=(count),
        in_specs=specs,
        out_specs=[pl.BlockSpec((bm, wide), lambda m: (first + m, 0))] * 3,
        out_shape=[jax.ShapeDtypeStruct((d, wide), jnp.bfloat16)] * 3,
        input_output_aliases=alias,
        compiler_params=_params(),
        cost_estimate=_cost(2 * rows * count * bm * 3 * wide, [a, *grads]),
        name="by_weights",
    )(*given)


def _permute(t, bit, n):
    return lax.ppermute(t, "tp", [(i, i ^ bit) for i in range(n)])


def gather(t, cuts, n):
    slots = {f"{kind}{s}": [] for kind in "id" for s in range(8)}
    for (first, size), route in zip(cuts, ROUTES):
        have = [(0, t[first : first + size])]
        for bit in route:
            for p, x in tuple(have):
                have.append((p ^ bit, _permute(x, bit, n)))
        for s, (p, x) in enumerate(have):
            slots[f"i{s}"].append((x, p, first))
            slots[f"d{s}"].append((_permute(x, 1, n), p ^ 1, first))
    return slots


def angles(place):
    half = HEAD // 2
    angle = place.astype(jnp.float32)[:, None] * THETA ** (-jnp.arange(half, dtype=jnp.float32) / half)
    cos, sin = jnp.cos(angle), jnp.sin(angle)
    return jnp.concatenate([cos, cos], 1), jnp.concatenate([-sin, sin], 1)


X_GROUPS = (("i0", "i1", "d0"), ("i2", "i4", "d1"), ("i3", "i5", "d2", "d4"), ("i6", "i7", "d3", "d5", "d6", "d7"))
Y_GROUPS = (("i0", "d0", "i1", "d1", "i2", "d2", "i4", "d4"), ("i3", "d3", "i5", "d5", "i6", "d6", "i7", "d7"))


def solution(mesh):
    n = mesh.shape["tp"]

    def step(x, dy, gain, wq, wk, wv, wo):
        me = lax.axis_index("tp")
        each, d = x.shape
        wide = x.astype(jnp.float32)
        scale = lax.rsqrt(jnp.mean(wide * wide, -1, keepdims=True) + 1e-6)
        gain32 = gain.astype(jnp.float32)
        a = (wide * scale * gain32).astype(jnp.bfloat16)

        def run(slots, groups, weights, turn, transposed, bk):
            out = whole = None
            for group in groups:
                group = [piece for slot in group for piece in slots[slot]]
                pos = (me ^ jnp.array([p for _, p, _ in group])) * each + jnp.array([first for _, _, first in group])
                turned = None
                if turn:
                    whose = [p for t, p, _ in group for _ in range(t.shape[0])]
                    row = [first + r for t, _, first in group for r in range(t.shape[0])]
                    place = (me ^ jnp.array(whose)) * each + jnp.array(row)
                    turned = angles(place)
                out, whole = project([t for t, _, _ in group], pos, weights, out, whole, turned, transposed, bk)
            return out, whole

        x_slots = gather(a, ((0, 48), (48, 48), (96, 32)), n)
        dy_slots = gather(dy, ((0, 32), (32, 48), (80, 48)), n)
        qkv, a_all = run(x_slots, X_GROUPS, (wq, wk, wv), True, False, 1024)
        seen, lse = attend(qkv)
        wo_then, _ = lax.optimization_barrier((wo, lse))
        d_seen, dy_all = run(dy_slots, Y_GROUPS, (wo_then,), False, True, 1024)
        cos, sin = angles(jnp.arange(n * each))
        grads = attend_back(qkv, d_seen, seen, lse, cos, sin)

        weights = (wq, wk, wv)
        bn = 512
        cuts = ((0, 5120), (5120, 4608), (9728, 4608))
        add = lambda u, v: u.astype(jnp.float32) + v.astype(jnp.float32)
        mine = []
        for (first, width), route in zip(cuts, ROUTES):
            order = [sum(b for k, b in enumerate(route) if i >> (2 - k) & 1) for i in range(8)]
            here = (me ^ jnp.array(order)) * each
            there = (me ^ jnp.array([p ^ 1 for p in order])) * each
            (term,) = by_rows(there, grads, weights, first, width, bn)
            got = _permute(term, 1, n)
            keep, send = by_rows(here, grads, weights, first, width, bn, got)
            for s, bit in enumerate(route):
                got = _permute(send, bit, n)
                rows = keep.shape[0]
                if s < 2:
                    send = add(keep[rows // 2 :], got[rows // 2 :]).astype(jnp.bfloat16)
                    keep = add(keep[: rows // 2], got[: rows // 2]).astype(jnp.bfloat16)
                else:
                    mine.append(add(keep, got))
        by_wo = lax.dot_general(seen, dy_all, (((0,), (0,)), ((), ())), preferred_element_type=jnp.float32).astype(jnp.bfloat16)
        by_w = None
        for first, count in ((0, 10), (10, 9), (19, 9)):
            by_w = by_weights(a_all, grads, first, count, by_w)
        by_wq, by_wk, by_wv = by_w

        dn = jnp.concatenate(mine, axis=1)
        part = dn * gain32
        inner = jnp.sum(part * wide, -1, keepdims=True) / d
        by_x = (dy.astype(jnp.float32) + scale * (part - wide * (scale * scale * inner))).astype(jnp.bfloat16)
        by_gain = jnp.sum(dn * (wide * scale), 0, keepdims=True)
        for bit in (8, 4, 2, 1):
            got = _permute(by_gain, bit, n)
            by_gain = by_gain + got
        return by_x, by_gain, by_wq, by_wk, by_wv, by_wo

    tokens, columns = P(("dp", "tp"), None), P(None, "tp")
    return jax.shard_map(
        step,
        mesh=mesh,
        in_specs=(tokens, tokens, P(None), columns, columns, columns, P("tp", None)),
        out_specs=(tokens, P("dp", None), P("dp", "tp"), P("dp", "tp"), P("dp", "tp"), P(("dp", "tp"), None)),
        check_vma=False,
    )
```
